32 devices in a mesh: expert: 2 (over x), dp: 16 (over z, y, core).
Axes of the slice: x: 2, y: 2, z: 4, core: 2. Of those that a mesh axis runs over, the one named last changes fastest.
Arguments:
- grads: bfloat16 [2, 16, 128, 6144], P('expert', 'dp'), may hold values from -16 to 16
- master: float32 [2, 128, 6144], P('expert', 'dp'), may hold values from -0.0625 to 0.0625
- first_moment: float32 [2, 128, 6144], P('expert', 'dp'), may hold values from -0.0029296875 to 0.0029296875
- second_moment: float32 [2, 128, 6144], P('expert', 'dp'), may hold values from 1e-08 to 1e-07
Outputs:
- new_master: float32 [2, 128, 6144], P('expert', 'dp')
- new_first: float32 [2, 128, 6144], P('expert', 'dp')
- new_second: float32 [2, 128, 6144], P('expert', 'dp')
- direction: float32 [2, 128, 6144], P('expert', 'dp')
- new_weights: bfloat16 [2, 128, 6144], P('expert')
The draws below stay inside these ranges and needn't reach their ends.
All inputs are finite; a program needn't handle non-finite values.
Results may differ from the reference program's by a relative error of at most 0.0004.
Values may be sent and summed in bfloat16 or wider, within the bound.
A program may use at most 64 MiB of HBM per device.

```python
import math
import jax
import jax.numpy as jnp
from jax import lax

D = 6144
ROWS = 128
STEP = 10
EXPERTS = 2
N_DP = 16


def draw_grads(key, part):
    key_common = jax.random.fold_in(key, 11)
    key_scale = jax.random.fold_in(key, 12)
    key_noise = jax.random.fold_in(key, 13)
    key_pairs = jax.random.fold_in(key, 14)
    rows_per = ROWS // N_DP
    row_scale = jnp.exp(jax.random.uniform(key_scale, (EXPERTS, 1, ROWS, 1), jnp.float32, math.log(0.5), math.log(2.0)))
    pairing = jax.random.permutation(key_pairs, N_DP)
    owner = jnp.arange(ROWS, dtype=jnp.int32) // rows_per
    spike = jnp.where(owner[None, :] == pairing[:, None], 4.0, 1.0).astype(jnp.float32)
    spike = spike.reshape(1, N_DP, ROWS, 1)
    common = 0.25 * row_scale * jax.random.truncated_normal(key_common, -4.0, 4.0, (EXPERTS, 1, ROWS, D), jnp.float32)
    noise = jax.random.truncated_normal(key_noise, -3.0, 3.0, (EXPERTS, N_DP, ROWS, D), jnp.float32)
    return (common + spike * noise).astype(jnp.bfloat16)


def block_levels(key, extent, cuts, least, largest):
    gain = 1.0
    for axis_at, parts in cuts:
        steps = jax.random.uniform(jax.random.fold_in(jax.random.fold_in(key, 6), axis_at), (parts,), jnp.float32, least / len(cuts), largest / len(cuts))
        gain = gain * jnp.repeat(jnp.exp(steps), extent[axis_at] // parts).reshape((-1,) + (1,) * (len(extent) - 1 - axis_at))
    return gain


def normal_values(stream_key, extent, deviation, most, shards=(), held_as=jnp.bfloat16):
    result = deviation * jax.random.normal(stream_key, extent, jnp.float32)
    if shards:
        result = result * block_levels(stream_key, extent, shards, -0.22, 0.18)
    return jnp.clip(result, -most, most).astype(held_as)


def setup_inputs(seed: int = 0) -> dict:
    seeds = jax.random.split(jax.random.key(seed), 5)
    return {
        "grads": draw_grads(jax.random.fold_in(seeds[4], 71), 0),
        "master": normal_values(seeds[1], (EXPERTS, ROWS, D), 0.004, 0.0625, ((0, 2), (1, 16)), jnp.float32),
        "first_moment": normal_values(seeds[2], (EXPERTS, ROWS, D), 0.0002, 0.0029296875, ((0, 2), (1, 16)), jnp.float32),
        "second_moment": jnp.clip(jnp.exp(math.log(1.0000000116860974e-07) - 2.3025851 * jax.random.uniform(seeds[3], (EXPERTS, ROWS, D), jnp.float32) ** block_levels(seeds[3], (EXPERTS, ROWS, D), ((0, 2), (1, 16)), -0.2, 0.2)), 9.99999993922529e-09, 1.0000000116860974e-07),
    }


def reference(grads, master, first_moment, second_moment):

    def add_one(index, total):
        piece = lax.dynamic_index_in_dim(grads, index, 1, keepdims=False)
        return total + piece.astype(jnp.float32)
    summed = lax.fori_loop(0, grads.shape[1], add_one, jnp.zeros(master.shape, jnp.float32))
    norm = jnp.sqrt(jnp.sum(summed * summed))
    clip = 1.0 / jnp.maximum(norm, 1.0)
    clipped = clip * summed
    new_first = 0.9 * first_moment + 0.1 * clipped
    new_second = 0.95 * second_moment + 0.05 * (clipped * clipped)
    first_fix = 1.0 - 0.9 ** STEP
    second_fix = 1.0 - 0.95 ** STEP
    direction = new_first / first_fix / (jnp.sqrt(new_second / second_fix) + 1e-08)
    new_master = master - 0.001 * (direction + 0.1 * master)
    new_weights = new_master.astype(jnp.bfloat16)
    return (new_master, new_first, new_second, direction, new_weights)
```

```python
import functools

import jax
import jax.numpy as jnp
from jax import lax
from jax.experimental import pallas as pl
from jax.experimental.pallas import tpu as pltpu
from jax.sharding import PartitionSpec as P

STEP = 10
MESH = pl.DeviceIdType.MESH


def factors(mesh):
    size = mesh.shape["dp"]
    row = mesh.devices.reshape(-1, size)[0]
    try:
        places = [tuple(d.coords) for d in row]
        cores = size // len(set(places))
        far = len({p[2] for p in places})
    except AttributeError:
        cores, far = 1, size
    return far, size // far // cores, cores


def pieces(width):
    half = width // 2 // 128 * 128
    return [(0, half), (half, width - half)] if half else [(0, width)]


def kernel(sizes, experts, grads, master, first, second, new_master, new_first, new_second, direction, weights,
           raw, own, part, got, master_v, first_v, second_v, norms,
           load_sem, raw_send, raw_recv, part_send, part_recv, norm_send, norm_recv,
           far_send, far_recv, near_send, near_recv, core_send, core_recv):
    A, Y, C = sizes
    B = Y * C
    n = A * B
    width = grads.shape[-1]
    cuts = pieces(width)
    e, me = lax.axis_index("expert"), lax.axis_index("dp")
    a, b = me // B, me % B
    y, c = b // C, b % C

    def turn(value, by, count):
        return (value + by) % count

    def at(za, yb, cc):
        return (e, za * B + yb * C + cc)

    inner = [(dy, dc) for dy in range(Y) for dc in range(C) if dy or dc]
    inner.sort(key=lambda t: -t[0])
    order = sorted(range(1, A), key=lambda k: -min(k, A - k)) + [0]
    everyone = [(de, dd) for de in range(experts) for dd in range(n) if de or dd]

    barrier = pltpu.get_barrier_semaphore()
    for de, dd in everyone:
        pl.semaphore_signal(barrier, inc=1, device_id=(turn(e, de, experts), turn(me, dd, n)), device_id_type=MESH)

    loads = [pltpu.make_async_copy(grads.at[:, b], own, load_sem.at[0])]
    for i, (src, dst) in enumerate(((master, master_v), (first, first_v), (second, second_v))):
        loads.append(pltpu.make_async_copy(src, dst, load_sem.at[i + 1]))
    for copy in loads:
        copy.start()
    pl.semaphore_wait(barrier, len(everyone))

    raws = {}
    for k in order:
        for h, (at0, wide) in enumerate(cuts):
            for i, (dy, dc) in enumerate(inner):
                y2, c2 = turn(y, dy, Y), turn(c, dc, C)
                copy = pltpu.make_async_remote_copy(
                    src_ref=grads.at[turn(a, k, A), y2 * C + c2, :, pl.ds(at0, wide)],
                    dst_ref=raw.at[i, k, :, pl.ds(at0, wide)],
                    send_sem=raw_send.at[i, k, h], recv_sem=raw_recv.at[i, k, h],
                    device_id=at(a, y2, c2), device_id_type=MESH)
                copy.start()
                raws[i, k, h] = copy
    loads[0].wait()

    parts = {}
    for k in order:
        far = turn(a, k, A)
        for h, (at0, wide) in enumerate(cuts):
            cols = pl.ds(at0, wide)
            total = own[far, :, cols].astype(jnp.float32)
            for i in range(len(inner)):
                raws[i, k, h].wait_recv()
                total = total + raw[i, k, :, cols].astype(jnp.float32)
            part[k, :, cols] = total
            if k:
                copy = pltpu.make_async_remote_copy(
                    src_ref=part.at[k, :, cols], dst_ref=got.at[k, :, cols],
                    send_sem=part_send.at[k, h], recv_sem=part_recv.at[k, h],
                    device_id=at(far, y, c), device_id_type=MESH)
                copy.start()
                parts[k, h] = copy

    square = jnp.zeros((1, 128), jnp.float32)
    for h, (at0, wide) in enumerate(cuts):
        cols = pl.ds(at0, wide)
        total = part[0, :, cols]
        for k in order[:-1]:
            parts[k, h].wait_recv()
            total = total + got[k, :, cols]
        part[0, :, cols] = total
        squares = jnp.sum(total * total, axis=0, keepdims=True)
        for j in range(wide // 128):
            square = square + squares[:, j * 128:(j + 1) * 128]
    norms[0] = square
    sent = []
    for i, (de, dd) in enumerate(everyone):
        copy = pltpu.make_async_remote_copy(
            src_ref=norms.at[0], dst_ref=norms.at[i + 1],
            send_sem=norm_send.at[i], recv_sem=norm_recv.at[i],
            device_id=(turn(e, de, experts), turn(me, dd, n)), device_id_type=MESH)
        copy.start()
        sent.append(copy)
    for copy in loads[1:]:
        copy.wait()
    for copy in sent:
        copy.wait_recv()
    whole = jnp.sum(jnp.sum(norms[...], axis=0), axis=1, keepdims=True)
    clip = 1.0 / jnp.maximum(jnp.sqrt(whole), 1.0)

    def forward(where, cols, send, recv, target):
        copy = pltpu.make_async_remote_copy(
            src_ref=weights.at[where[0], where[1], :, cols], dst_ref=weights.at[where[0], where[1], :, cols],
            send_sem=send, recv_sem=recv, device_id=target, device_id_type=MESH)
        copy.start()
        return copy

    fars, nears, partners = {}, {}, {}

    def to_near(k, h, cols):
        for dy in range(1, Y):
            nears[dy, k, h] = forward((turn(a, -k, A), b), cols, near_send.at[dy - 1, k, h], near_recv.at[dy - 1, k, h],
                                      at(a, turn(y, dy, Y), c))

    def to_core(dy, k, h, cols):
        for dc in range(1, C):
            partners[dc, dy, k, h] = forward((turn(a, -k, A), turn(y, -dy, Y) * C + c), cols,
                                             core_send.at[dc - 1, dy, k, h], core_recv.at[dc - 1, dy, k, h],
                                             at(a, y, turn(c, dc, C)))

    first_fix = 1.0 / (1.0 - 0.9**STEP)
    second_fix = 1.0 / (1.0 - 0.95**STEP)
    for h, (at0, wide) in enumerate(cuts):
        cols = pl.ds(at0, wide)
        clipped = clip * part[0, :, cols]
        m = 0.9 * first_v[:, cols] + 0.1 * clipped
        v = 0.95 * second_v[:, cols] + 0.05 * (clipped * clipped)
        d = (m * first_fix) / (jnp.sqrt(v * second_fix) + 1e-08)
        w = master_v[:, cols]
        w = w - 0.001 * (d + 0.1 * w)
        weights[a, b, :, cols] = w.astype(jnp.bfloat16)
        new_master[:, cols] = w
        new_first[:, cols] = m
        new_second[:, cols] = v
        direction[:, cols] = d
        to_near(0, h, cols)
        for k in order[:-1]:
            fars[k, h] = forward((a, b), cols, far_send.at[k, h], far_recv.at[k, h], at(turn(a, k, A), y, c))
        to_core(0, 0, h, cols)
    near_first = sorted(range(1, A), key=lambda k: min(k, A - k))
    for k in near_first:
        for h, (at0, wide) in enumerate(cuts):
            cols = pl.ds(at0, wide)
            fars[k, h].wait_recv()
            to_near(k, h, cols)
            to_core(0, k, h, cols)
    for k in [0] + near_first:
        for h, (at0, wide) in enumerate(cuts):
            cols = pl.ds(at0, wide)
            for dy in range(1, Y):
                nears[dy, k, h].wait_recv()
                to_core(dy, k, h, cols)
    for copy in partners.values():
        copy.wait_recv()
    for copies in (raws, parts, fars, nears, partners):
        for copy in copies.values():
            copy.wait_send()
    for copy in sent:
        copy.wait_send()


def solution(mesh):
    A, Y, C = factors(mesh)
    B = Y * C
    experts = mesh.shape["expert"]
    n = A * B

    def shards(grads, master, first_moment, second_moment):
        rows, width = master.shape[1:]
        H = len(pieces(width))
        state = jax.ShapeDtypeStruct((rows, width), jnp.float32)
        dma = pltpu.SemaphoreType.DMA
        many = experts * n - 1
        vmem = pl.BlockSpec(memory_space=pltpu.VMEM)
        hbm = pl.BlockSpec(memory_space=pl.ANY)
        outs = pl.pallas_call(
            functools.partial(kernel, (A, Y, C), experts),
            out_shape=(state, state, state, state, jax.ShapeDtypeStruct((A, B, rows, width), jnp.bfloat16)),
            in_specs=[hbm] * 4,
            out_specs=(vmem,) * 5,
            scratch_shapes=[
                pltpu.VMEM((max(B - 1, 1), A, rows, width), jnp.bfloat16),
                pltpu.VMEM((A, rows, width), jnp.bfloat16),
                pltpu.VMEM((A, rows, width), jnp.float32),
                pltpu.VMEM((A, rows, width), jnp.float32),
                pltpu.VMEM((rows, width), jnp.float32),
                pltpu.VMEM((rows, width), jnp.float32),
                pltpu.VMEM((rows, width), jnp.float32),
                pltpu.VMEM((many + 1, 1, 128), jnp.float32),
                dma((4,)),
                dma((max(B - 1, 1), A, H)), dma((max(B - 1, 1), A, H)),
                dma((A, H)), dma((A, H)),
                dma((many,)), dma((many,)),
                dma((A, H)), dma((A, H)),
                dma((max(Y - 1, 1), A, H)), dma((max(Y - 1, 1), A, H)),
                dma((max(C - 1, 1), Y, A, H)), dma((max(C - 1, 1), Y, A, H)),
            ],
            compiler_params=pltpu.CompilerParams(collective_id=0, has_side_effects=True),
        )(grads.reshape(A, B, rows, width), master[0], first_moment[0], second_moment[0])
        return tuple(x[None] for x in outs[:4]) + (outs[4].reshape(1, n * rows, width),)

    split = P("expert", "dp", None)
    return jax.shard_map(shards, mesh=mesh, in_specs=(P("expert", "dp", None, None), split, split, split),
                         out_specs=(split, split, split, split, P("expert", None, None)), check_vma=False)
```

```python
import functools

import jax
import jax.numpy as jnp
from jax import lax
from jax.experimental import pallas as pl
from jax.experimental.pallas import tpu as pltpu
from jax.sharding import PartitionSpec as P

STEP = 10
MESH = pl.DeviceIdType.MESH


def factors(mesh):
    size = mesh.shape["dp"]
    row = mesh.devices.reshape(-1, size)[0]
    try:
        places = [tuple(d.coords) for d in row]
        cores = size // len(set(places))
        far = len({p[2] for p in places})
    except AttributeError:
        cores, far = 1, size
    return far, size // far // cores, cores


def pieces(width):
    half = width // 2 // 128 * 128
    return [(0, half), (half, width - half)] if half else [(0, width)]


def kernel(sizes, experts, grads, master, first, second, new_master, new_first, new_second, direction, weights,
           raw, own, part, got, master_v, first_v, second_v, norms,
           load_sem, raw_send, raw_recv, part_send, part_recv, norm_send, norm_recv,
           far_send, far_recv, near_send, near_recv, core_send, core_recv):
    A, Y, C = sizes
    B = Y * C
    n = A * B
    width = grads.shape[-1]
    cuts = pieces(width)
    e, me = lax.axis_index("expert"), lax.axis_index("dp")
    a, b = me // B, me % B
    y, c = b // C, b % C

    def turn(value, by, count):
        return (value + by) % count

    def at(za, yb, cc):
        return (e, za * B + yb * C + cc)

    inner = [(dy, dc) for dy in range(Y) for dc in range(C) if dy or dc]
    inner.sort(key=lambda t: -t[0])
    order = sorted(range(1, A), key=lambda k: -min(k, A - k)) + [0]
    everyone = [(de, dd) for de in range(experts) for dd in range(n) if de or dd]

    barrier = pltpu.get_barrier_semaphore()
    for de, dd in everyone:
        pl.semaphore_signal(barrier, inc=1, device_id=(turn(e, de, experts), turn(me, dd, n)), device_id_type=MESH)

    loads = [pltpu.make_async_copy(grads.at[:, b], own, load_sem.at[0])]
    for i, (src, dst) in enumerate(((master, master_v), (first, first_v), (second, second_v))):
        loads.append(pltpu.make_async_copy(src, dst, load_sem.at[i + 1]))
    for copy in loads:
        copy.start()
    pl.semaphore_wait(barrier, len(everyone))

    raws = {}
    for k in order:
        for h, (at0, wide) in enumerate(cuts):
            for i, (dy, dc) in enumerate(inner):
                y2, c2 = turn(y, dy, Y), turn(c, dc, C)
                copy = pltpu.make_async_remote_copy(
                    src_ref=grads.at[turn(a, k, A), y2 * C + c2, :, pl.ds(at0, wide)],
                    dst_ref=raw.at[i, k, :, pl.ds(at0, wide)],
                    send_sem=raw_send.at[i, k, h], recv_sem=raw_recv.at[i, k, h],
                    device_id=at(a, y2, c2), device_id_type=MESH)
                copy.start()
                raws[i, k, h] = copy
    loads[0].wait()

    parts = {}
    for k in order:
        far = turn(a, k, A)
        for h, (at0, wide) in enumerate(cuts):
            cols = pl.ds(at0, wide)
            total = own[far, :, cols].astype(jnp.float32)
            for i in range(len(inner)):
                raws[i, k, h].wait_recv()
                total = total + raw[i, k, :, cols].astype(jnp.float32)
            part[k, :, cols] = total
            if k:
                copy = pltpu.make_async_remote_copy(
                    src_ref=part.at[k, :, cols], dst_ref=got.at[k, :, cols],
                    send_sem=part_send.at[k, h], recv_sem=part_recv.at[k, h],
                    device_id=at(far, y, c), device_id_type=MESH)
                copy.start()
                parts[k, h] = copy

    square = jnp.zeros((1, 128), jnp.float32)
    for h, (at0, wide) in enumerate(cuts):
        cols = pl.ds(at0, wide)
        total = part[0, :, cols]
        for k in order[:-1]:
            parts[k, h].wait_recv()
            total = total + got[k, :, cols]
        part[0, :, cols] = total
        squares = jnp.sum(total * total, axis=0, keepdims=True)
        for j in range(wide // 128):
            square = square + squares[:, j * 128:(j + 1) * 128]
    norms[0] = square
    sent = []
    for i, (de, dd) in enumerate(everyone):
        copy = pltpu.make_async_remote_copy(
            src_ref=norms.at[0], dst_ref=norms.at[i + 1],
            send_sem=norm_send.at[i], recv_sem=norm_recv.at[i],
            device_id=(turn(e, de, experts), turn(me, dd, n)), device_id_type=MESH)
        copy.start()
        sent.append(copy)
    for copy in loads[1:]:
        copy.wait()
    for copy in sent:
        copy.wait_recv()
    whole = jnp.sum(jnp.sum(norms[...], axis=0), axis=1, keepdims=True)
    clip = 1.0 / jnp.maximum(jnp.sqrt(whole), 1.0)

    def forward(where, cols, send, recv, target):
        copy = pltpu.make_async_remote_copy(
            src_ref=weights.at[where[0], where[1], :, cols], dst_ref=weights.at[where[0], where[1], :, cols],
            send_sem=send, recv_sem=recv, device_id=target, device_id_type=MESH)
        copy.start()
        return copy

    fars, nears, partners = {}, {}, {}

    def to_near(k, h, cols):
        for dy in range(1, Y):
            nears[dy, k, h] = forward((turn(a, -k, A), b), cols, near_send.at[dy - 1, k, h], near_recv.at[dy - 1, k, h],
                                      at(a, turn(y, dy, Y), c))

    def to_core(dy, k, h, cols):
        for dc in range(1, C):
            partners[dc, dy, k, h] = forward((turn(a, -k, A), turn(y, -dy, Y) * C + c), cols,
                                             core_send.at[dc - 1, dy, k, h], core_recv.at[dc - 1, dy, k, h],
                                             at(a, y, turn(c, dc, C)))

    first_fix = 1.0 / (1.0 - 0.9**STEP)
    second_fix = 1.0 / (1.0 - 0.95**STEP)
    for h, (at0, wide) in enumerate(cuts):
        cols = pl.ds(at0, wide)
        clipped = clip * part[0, :, cols]
        m = 0.9 * first_v[:, cols] + 0.1 * clipped
        v = 0.95 * second_v[:, cols] + 0.05 * (clipped * clipped)
        d = (m * first_fix) / (jnp.sqrt(v * second_fix) + 1e-08)
        w = master_v[:, cols]
        w = w - 0.001 * (d + 0.1 * w)
        weights[a, b, :, cols] = w.astype(jnp.bfloat16)
        new_master[:, cols] = w
        new_first[:, cols] = m
        new_second[:, cols] = v
        direction[:, cols] = d
        to_near(0, h, cols)
        for k in order[:-1]:
            fars[k, h] = forward((a, b), cols, far_send.at[k, h], far_recv.at[k, h], at(turn(a, k, A), y, c))
        to_core(0, 0, h, cols)
    near_first = sorted(range(1, A), key=lambda k: min(k, A - k))
    for k in near_first:
        for h, (at0, wide) in enumerate(cuts):
            cols = pl.ds(at0, wide)
            fars[k, h].wait_recv()
            to_near(k, h, cols)
            to_core(0, k, h, cols)
    for k in [0] + near_first:
        for h, (at0, wide) in enumerate(cuts):
            cols = pl.ds(at0, wide)
            for dy in range(1, Y):
                nears[dy, k, h].wait_recv()
                to_core(dy, k, h, cols)
    for copy in partners.values():
        copy.wait_recv()
    for copies in (raws, parts, fars, nears, partners):
        for copy in copies.values():
            copy.wait_send()
    for copy in sent:
        copy.wait_send()


def solution(mesh):
    A, Y, C = factors(mesh)
    B = Y * C
    experts = mesh.shape["expert"]
    n = A * B

    def shards(grads, master, first_moment, second_moment):
        rows, width = master.shape[1:]
        H = len(pieces(width))
        dma = pltpu.SemaphoreType.DMA
        many = experts * n - 1
        vmem = pl.BlockSpec(memory_space=pltpu.VMEM)
        hbm = pl.BlockSpec(memory_space=pl.ANY)
        outs = pl.pallas_call(
            functools.partial(kernel, (A, Y, C), experts),
            out_shape=(pltpu.VMEM((rows, width), jnp.float32),) * 4 + (pltpu.VMEM((A, B, rows, width), jnp.bfloat16),),
            in_specs=[hbm] * 4,
            out_specs=(vmem,) * 5,
            scratch_shapes=[
                pltpu.VMEM((max(B - 1, 1), A, rows, width), jnp.bfloat16),
                pltpu.VMEM((A, rows, width), jnp.bfloat16),
                pltpu.VMEM((A, rows, width), jnp.float32),
                pltpu.VMEM((A, rows, width), jnp.float32),
                pltpu.VMEM((rows, width), jnp.float32),
                pltpu.VMEM((rows, width), jnp.float32),
                pltpu.VMEM((rows, width), jnp.float32),
                pltpu.VMEM((many + 1, 1, 128), jnp.float32),
                dma((4,)),
                dma((max(B - 1, 1), A, H)), dma((max(B - 1, 1), A, H)),
                dma((A, H)), dma((A, H)),
                dma((many,)), dma((many,)),
                dma((A, H)), dma((A, H)),
                dma((max(Y - 1, 1), A, H)), dma((max(Y - 1, 1), A, H)),
                dma((max(C - 1, 1), Y, A, H)), dma((max(C - 1, 1), Y, A, H)),
            ],
            compiler_params=pltpu.CompilerParams(collective_id=0, has_side_effects=True),
        )(grads.reshape(A, B, rows, width), master[0], first_moment[0], second_moment[0])
        return tuple(x[None] for x in outs[:4]) + (outs[4].reshape(1, n * rows, width),)

    split = P("expert", "dp", None)
    return jax.shard_map(shards, mesh=mesh, in_specs=(P("expert", "dp", None, None), split, split, split),
                         out_specs=(split, split, split, split, P("expert", None, None)), check_vma=False)
```

```python
import functools

import jax
import jax.numpy as jnp
from jax import lax
from jax.experimental import pallas as pl
from jax.experimental.pallas import tpu as pltpu
from jax.sharding import PartitionSpec as P

STEP = 10
CUTS = 3
MESH = pl.DeviceIdType.MESH


def factors(mesh):
    size = mesh.shape["dp"]
    row = mesh.devices.reshape(-1, size)[0]
    try:
        places = [tuple(d.coords) for d in row]
        cores = size // len(set(places))
        far = len({p[2] for p in places})
    except AttributeError:
        cores, far = 1, size
    return far, size // far // cores, cores


def pieces(width):
    tiles = width // 128
    edges = [tiles * i // CUTS * 128 for i in range(CUTS)] + [width]
    return [(p, q - p) for p, q in zip(edges, edges[1:]) if q > p]


def kernel(sizes, experts, grads, master, first, second, new_master, new_first, new_second, direction, weights,
           raw, own, part, arrived, master_v, first_v, second_v, norms,
           load_sem, raw_send, raw_recv, part_send, part_recv, norm_send, norm_recv,
           far_send, far_recv, near_send, near_recv, core_send, core_recv):
    A, Y, C = sizes
    B = Y * C
    n = A * B
    width = grads.shape[-1]
    cuts = pieces(width)
    e, me = lax.axis_index("expert"), lax.axis_index("dp")
    a, b = me // B, me % B
    y, c = b // C, b % C

    def turn(value, by, count):
        return (value + by) % count

    def at(za, yb, cc):
        return (e, za * B + yb * C + cc)

    inner = [(dy, dc) for dy in range(Y) for dc in range(C) if dy or dc]
    inner.sort(key=lambda t: -t[0])
    table = [sorted(range(A), key=lambda t: (-abs(t - z), t)) for z in range(A)]

    def chosen(row):
        pick = row[0]
        for z in range(1, A):
            pick = jnp.where(a == z, row[z], pick)
        return pick

    targets = [chosen([table[z][s] for z in range(A)]) for s in range(A - 1)] + [a]
    everyone = [(de, dd) for de in range(experts) for dd in range(n) if de or dd]

    barrier = pltpu.get_barrier_semaphore()

    def greet(device):
        pl.semaphore_signal(barrier, inc=1, device_id=device, device_id_type=MESH)

    for dy, dc in inner:
        greet(at(a, turn(y, dy, Y), turn(c, dc, C)))
    for de in range(1, experts):
        greet((turn(e, de, experts), me))
    pl.when(a > 0)(lambda: greet(at(a - 1, y, c)))
    pl.when(a < A - 1)(lambda: greet(at(a + 1, y, c)))
    greeted = len(inner) + experts - 1 + jnp.where(a > 0, 1, 0) + jnp.where(a < A - 1, 1, 0)

    loads = [pltpu.make_async_copy(grads.at[:, b], own, load_sem.at[0])]
    for i, (src, dst) in enumerate(((master, master_v), (first, first_v), (second, second_v))):
        loads.append(pltpu.make_async_copy(src, dst, load_sem.at[i + 1]))
    for copy in loads:
        copy.start()
    pl.semaphore_wait(barrier, greeted)

    raws = {}
    for s, t in enumerate(targets):
        for h, (at0, wide) in enumerate(cuts):
            for i, (dy, dc) in enumerate(inner):
                y2, c2 = turn(y, dy, Y), turn(c, dc, C)
                copy = pltpu.make_async_remote_copy(
                    src_ref=grads.at[t, y2 * C + c2, :, pl.ds(at0, wide)],
                    dst_ref=raw.at[i, s, :, pl.ds(at0, wide)],
                    send_sem=raw_send.at[i, s, h], recv_sem=raw_recv.at[i, s, h],
                    device_id=at(a, y2, c2), device_id_type=MESH)
                copy.start()
                raws[i, s, h] = copy
    loads[0].wait()

    def step_on(d, s, t, h):
        cols = pl.ds(*cuts[h])
        ahead = jnp.where(d == 0, jnp.minimum(a + 1, A - 1), jnp.maximum(a - 1, 0))
        return pltpu.make_async_remote_copy(
            src_ref=part.at[s, :, cols], dst_ref=arrived.at[d, t, :, cols],
            send_sem=part_send.at[s, h], recv_sem=part_recv.at[d, t, h],
            device_id=at(ahead, y, c), device_id_type=MESH)

    def add_arrived(d, s, t, h):
        cols = pl.ds(*cuts[h])
        step_on(d, s, t, h).wait_recv()
        part[s, :, cols] = part[s, :, cols] + arrived[d, t, :, cols]

    parts = {}
    square = jnp.zeros((1, 128), jnp.float32)
    for s, t in enumerate(targets):
        for h, (at0, wide) in enumerate(cuts):
            cols = pl.ds(at0, wide)
            total = own[t, :, cols].astype(jnp.float32)
            for i in range(len(inner)):
                raws[i, s, h].wait_recv()
                total = total + raw[i, s, :, cols].astype(jnp.float32)
            part[s, :, cols] = total
            if s < A - 1:
                d = jnp.where(t > a, 0, 1)
                behind = jnp.where(t > a, a, A - 1 - a)
                pl.when(behind > 0)(functools.partial(add_arrived, d, s, t, h))
                parts[s, h] = step_on(d, s, t, h)
                parts[s, h].start()
            else:
                pl.when(a > 0)(functools.partial(add_arrived, 0, s, t, h))
                pl.when(a < A - 1)(functools.partial(add_arrived, 1, s, t, h))
                total = part[s, :, cols]
                squares = jnp.sum(total * total, axis=0, keepdims=True)
                for j in range(wide // 128):
                    square = square + squares[:, j * 128:(j + 1) * 128]
    norms[0] = square
    sent = []
    for i, (de, dd) in enumerate(everyone):
        copy = pltpu.make_async_remote_copy(
            src_ref=norms.at[0], dst_ref=norms.at[i + 1],
            send_sem=norm_send.at[i], recv_sem=norm_recv.at[i],
            device_id=(turn(e, de, experts), turn(me, dd, n)), device_id_type=MESH)
        copy.start()
        sent.append(copy)
    for copy in loads[1:]:
        copy.wait()
    for copy in sent:
        copy.wait_recv()
    whole = jnp.sum(jnp.sum(norms[...], axis=0), axis=1, keepdims=True)
    clip = 1.0 / jnp.maximum(jnp.sqrt(whole), 1.0)

    def forward(where, cols, send, recv, target):
        copy = pltpu.make_async_remote_copy(
            src_ref=weights.at[where[0], where[1], :, cols], dst_ref=weights.at[where[0], where[1], :, cols],
            send_sem=send, recv_sem=recv, device_id=target, device_id_type=MESH)
        return copy

    places = {0: (a, True)}
    for dist in range(1, A):
        places[2 * dist - 1] = (a - dist, a >= dist)
        places[2 * dist] = (a + dist, a + dist < A)

    def near_copy(dy, slot, h):
        where = jnp.clip(places[slot][0], 0, A - 1)
        return forward((where, b), pl.ds(*cuts[h]), near_send.at[dy - 1, slot, h],
                       near_recv.at[dy - 1, slot, h], at(a, turn(y, dy, Y), c))

    def core_copy(dc, dy, slot, h):
        where = jnp.clip(places[slot][0], 0, A - 1)
        return forward((where, turn(y, -dy, Y) * C + c), pl.ds(*cuts[h]), core_send.at[dc - 1, dy, slot, h],
                       core_recv.at[dc - 1, dy, slot, h], at(a, y, turn(c, dc, C)))

    def to_near(slot, h):
        for dy in range(1, Y):
            near_copy(dy, slot, h).start()

    def to_core(dy, slot, h):
        for dc in range(1, C):
            core_copy(dc, dy, slot, h).start()

    def along(slot, up, hop, h):
        dist = (slot + 1) // 2 + hop
        where = jnp.clip(places[slot][0], 0, A - 1)
        there = jnp.minimum(a + hop, A - 1) if up else jnp.maximum(a - hop, 0)
        return pltpu.make_async_remote_copy(
            src_ref=weights.at[where, b, :, pl.ds(*cuts[h])], dst_ref=weights.at[where, b, :, pl.ds(*cuts[h])],
            send_sem=far_send.at[0 if up else 1, dist, h], recv_sem=far_recv.at[0 if up else 1, dist, h],
            device_id=at(there, y, c), device_id_type=MESH)

    def relay(slot, up, h, act="start"):
        dist = (slot + 1) // 2
        if dist % 2:
            return
        for hop in (2, 1):
            if dist + hop < A:
                here = (a + hop < A) if up else (a - hop >= 0)
                pl.when(here)(lambda hop=hop: getattr(along(slot, up, hop, h), act)())

    first_fix = 1.0 / (1.0 - 0.9**STEP)
    second_fix = 1.0 / (1.0 - 0.95**STEP)
    for h, (at0, wide) in enumerate(cuts):
        cols = pl.ds(at0, wide)
        clipped = clip * part[A - 1, :, cols]
        m = 0.9 * first_v[:, cols] + 0.1 * clipped
        v = 0.95 * second_v[:, cols] + 0.05 * (clipped * clipped)
        d = (m * first_fix) / (jnp.sqrt(v * second_fix) + 1e-08)
        w = master_v[:, cols]
        w = w - 0.001 * (d + 0.1 * w)
        weights[a, b, :, cols] = w.astype(jnp.bfloat16)
        new_master[:, cols] = w
        new_first[:, cols] = m
        new_second[:, cols] = v
        direction[:, cols] = d
        to_near(0, h)
        relay(0, True, h)
        relay(0, False, h)
        to_core(0, 0, h)

    def got_far(slot, h):
        dist = (slot + 1) // 2
        up = slot % 2 == 1
        hop = 1 if dist % 2 else 2
        where = jnp.clip(places[slot][0], 0, A - 1)
        block = weights.at[where, b, :, pl.ds(*cuts[h])]
        pltpu.make_async_remote_copy(
            src_ref=block, dst_ref=block, send_sem=far_send.at[0 if up else 1, dist, h],
            recv_sem=far_recv.at[0 if up else 1, dist, h],
            device_id=at(jnp.maximum(a - hop, 0) if up else jnp.minimum(a + hop, A - 1), y, c),
            device_id_type=MESH).wait_recv()
        to_near(slot, h)
        relay(slot, up, h)
        to_core(0, slot, h)

    def got_near(slot, h):
        for dy in range(1, Y):
            near_copy(dy, slot, h).wait_recv()
            to_core(dy, slot, h)

    def got_core(slot, h):
        for dc in range(1, C):
            for dy in range(Y):
                core_copy(dc, dy, slot, h).wait()
        for dy in range(1, Y):
            near_copy(dy, slot, h).wait_send()
        if slot == 0 or slot % 2:
            relay(slot, True, h, "wait_send")
        if slot % 2 == 0:
            relay(slot, False, h, "wait_send")

    slots = sorted(places, key=lambda k: (k + 1) // 2)
    steps = [(slot, h) for slot in slots for h in range(len(cuts))]
    lag = len(cuts) * 2

    def when(slot, work, h):
        if slot:
            pl.when(places[slot][1])(functools.partial(work, slot, h))
        else:
            work(slot, h)

    for i in range(len(steps) + lag):
        if i < len(steps) and steps[i][0]:
            when(steps[i][0], got_far, steps[i][1])
        if i >= lag:
            when(steps[i - lag][0], got_near, steps[i - lag][1])
    for slot, h in steps:
        when(slot, got_core, h)
    for copies in (raws, parts):
        for copy in copies.values():
            copy.wait_send()
    for copy in sent:
        copy.wait_send()


def solution(mesh):
    A, Y, C = factors(mesh)
    B = Y * C
    experts = mesh.shape["expert"]
    n = A * B

    def shards(grads, master, first_moment, second_moment):
        rows, width = master.shape[1:]
        H = len(pieces(width))
        dma = pltpu.SemaphoreType.DMA
        many = experts * n - 1
        vmem = pl.BlockSpec(memory_space=pltpu.VMEM)
        hbm = pl.BlockSpec(memory_space=pl.ANY)
        outs = pl.pallas_call(
            functools.partial(kernel, (A, Y, C), experts),
            out_shape=(pltpu.VMEM((rows, width), jnp.float32),) * 4 + (pltpu.VMEM((A, B, rows, width), jnp.bfloat16),),
            in_specs=[hbm] * 4,
            out_specs=(vmem,) * 5,
            scratch_shapes=[
                pltpu.VMEM((max(B - 1, 1), A, rows, width), jnp.bfloat16),
                pltpu.VMEM((A, rows, width), jnp.bfloat16),
                pltpu.VMEM((A, rows, width), jnp.float32),
                pltpu.VMEM((2, A, rows, width), jnp.float32),
                pltpu.VMEM((rows, width), jnp.float32),
                pltpu.VMEM((rows, width), jnp.float32),
                pltpu.VMEM((rows, width), jnp.float32),
                pltpu.VMEM((many + 1, 1, 128), jnp.float32),
                dma((4,)),
                dma((max(B - 1, 1), A, H)), dma((max(B - 1, 1), A, H)),
                dma((A, H)), dma((2, A, H)),
                dma((many,)), dma((many,)),
                dma((2, A, H)), dma((2, A, H)),
                dma((max(Y - 1, 1), 2 * A - 1, H)), dma((max(Y - 1, 1), 2 * A - 1, H)),
                dma((max(C - 1, 1), Y, 2 * A - 1, H)), dma((max(C - 1, 1), Y, 2 * A - 1, H)),
            ],
            compiler_params=pltpu.CompilerParams(collective_id=0, has_side_effects=True),
        )(grads.reshape(A, B, rows, width), master[0], first_moment[0], second_moment[0])
        return tuple(x[None] for x in outs[:4]) + (outs[4].reshape(1, n * rows, width),)

    split = P("expert", "dp", None)
    return jax.shard_map(shards, mesh=mesh, in_specs=(P("expert", "dp", None, None), split, split, split),
                         out_specs=(split, split, split, split, P("expert", None, None)), check_vma=False)
```

```python
import functools

import jax
import jax.numpy as jnp
from jax import lax
from jax.experimental import pallas as pl
from jax.experimental.pallas import tpu as pltpu
from jax.sharding import PartitionSpec as P

STEP = 10
CUTS = 2
MESH = pl.DeviceIdType.MESH


def factors(mesh):
    size = mesh.shape["dp"]
    row = mesh.devices.reshape(-1, size)[0]
    try:
        places = [tuple(d.coords) for d in row]
        cores = size // len(set(places))
        far = len({p[2] for p in places})
    except AttributeError:
        cores, far = 1, size
    return far, size // far // cores, cores


def pieces(width):
    tiles = width // 128
    edges = [tiles * i // CUTS * 128 for i in range(CUTS)] + [width]
    return [(p, q - p) for p, q in zip(edges, edges[1:]) if q > p]


def kernel(sizes, experts, grads, master, first, second, new_master, new_first, new_second, direction, weights,
           raw, own, part, arrived, master_v, first_v, second_v, norms,
           load_sem, raw_send, raw_recv, part_send, part_recv, norm_send, norm_recv,
           far_send, far_recv, near_send, near_recv, core_send, core_recv):
    A, Y, C = sizes
    B = Y * C
    n = A * B
    width = grads.shape[-1]
    cuts = pieces(width)
    e, me = lax.axis_index("expert"), lax.axis_index("dp")
    a, b = me // B, me % B
    y, c = b // C, b % C

    def turn(value, by, count):
        return (value + by) % count

    def at(za, yb, cc):
        return (e, za * B + yb * C + cc)

    inner = [(dy, dc) for dy in range(Y) for dc in range(C) if dy or dc]
    inner.sort(key=lambda t: -t[0])
    table = [sorted(range(A), key=lambda t: (-abs(t - z), t)) for z in range(A)]

    def chosen(row):
        pick = row[0]
        for z in range(1, A):
            pick = jnp.where(a == z, row[z], pick)
        return pick

    targets = [chosen([table[z][s] for z in range(A)]) for s in range(A - 1)] + [a]
    everyone = [(de, dd) for de in range(experts) for dd in range(n) if de or dd]

    barrier = pltpu.get_barrier_semaphore()

    def greet(device):
        pl.semaphore_signal(barrier, inc=1, device_id=device, device_id_type=MESH)

    for dy, dc in inner:
        greet(at(a, turn(y, dy, Y), turn(c, dc, C)))
    for de in range(1, experts):
        greet((turn(e, de, experts), me))
    pl.when(a > 0)(lambda: greet(at(a - 1, y, c)))
    pl.when(a < A - 1)(lambda: greet(at(a + 1, y, c)))
    greeted = len(inner) + experts - 1 + jnp.where(a > 0, 1, 0) + jnp.where(a < A - 1, 1, 0)

    loads = [pltpu.make_async_copy(grads.at[:, b], own, load_sem.at[0])]
    for i, (src, dst) in enumerate(((master, master_v), (first, first_v), (second, second_v))):
        loads.append(pltpu.make_async_copy(src, dst, load_sem.at[i + 1]))
    for copy in loads:
        copy.start()
    pl.semaphore_wait(barrier, greeted)

    raws = {}
    for s, t in enumerate(targets):
        for h, (at0, wide) in enumerate(cuts):
            for i, (dy, dc) in enumerate(inner):
                y2, c2 = turn(y, dy, Y), turn(c, dc, C)
                copy = pltpu.make_async_remote_copy(
                    src_ref=grads.at[t, y2 * C + c2, :, pl.ds(at0, wide)],
                    dst_ref=raw.at[i, s, :, pl.ds(at0, wide)],
                    send_sem=raw_send.at[i, s, h], recv_sem=raw_recv.at[i, s, h],
                    device_id=at(a, y2, c2), device_id_type=MESH)
                copy.start()
                raws[i, s, h] = copy
    loads[0].wait()

    def step_on(d, s, t, h):
        cols = pl.ds(*cuts[h])
        ahead = jnp.where(d == 0, jnp.minimum(a + 1, A - 1), jnp.maximum(a - 1, 0))
        return pltpu.make_async_remote_copy(
            src_ref=part.at[s, :, cols], dst_ref=arrived.at[d, t, :, cols],
            send_sem=part_send.at[s, h], recv_sem=part_recv.at[d, t, h],
            device_id=at(ahead, y, c), device_id_type=MESH)

    def add_arrived(d, s, t, h):
        cols = pl.ds(*cuts[h])
        step_on(d, s, t, h).wait_recv()
        part[s, :, cols] = part[s, :, cols] + arrived[d, t, :, cols]

    parts = {}
    square = jnp.zeros((1, 128), jnp.float32)
    for s, t in enumerate(targets):
        for h, (at0, wide) in enumerate(cuts):
            cols = pl.ds(at0, wide)
            total = own[t, :, cols].astype(jnp.float32)
            for i in range(len(inner)):
                raws[i, s, h].wait_recv()
                total = total + raw[i, s, :, cols].astype(jnp.float32)
            part[s, :, cols] = total
            if s < A - 1:
                d = jnp.where(t > a, 0, 1)
                behind = jnp.where(t > a, a, A - 1 - a)
                pl.when(behind > 0)(functools.partial(add_arrived, d, s, t, h))
                parts[s, h] = step_on(d, s, t, h)
                parts[s, h].start()
            else:
                pl.when(a > 0)(functools.partial(add_arrived, 0, s, t, h))
                pl.when(a < A - 1)(functools.partial(add_arrived, 1, s, t, h))
                total = part[s, :, cols]
                squares = jnp.sum(total * total, axis=0, keepdims=True)
                for j in range(wide // 128):
                    square = square + squares[:, j * 128:(j + 1) * 128]
    norms[0] = square
    sent = []
    for i, (de, dd) in enumerate(everyone):
        copy = pltpu.make_async_remote_copy(
            src_ref=norms.at[0], dst_ref=norms.at[i + 1],
            send_sem=norm_send.at[i], recv_sem=norm_recv.at[i],
            device_id=(turn(e, de, experts), turn(me, dd, n)), device_id_type=MESH)
        copy.start()
        sent.append(copy)
    for copy in loads[1:]:
        copy.wait()
    for copy in sent:
        copy.wait_recv()
    whole = jnp.sum(jnp.sum(norms[...], axis=0), axis=1, keepdims=True)
    clip = 1.0 / jnp.maximum(jnp.sqrt(whole), 1.0)

    def forward(where, cols, send, recv, target):
        copy = pltpu.make_async_remote_copy(
            src_ref=weights.at[where[0], where[1], :, cols], dst_ref=weights.at[where[0], where[1], :, cols],
            send_sem=send, recv_sem=recv, device_id=target, device_id_type=MESH)
        return copy

    places = {0: (a, True)}
    for dist in range(1, A):
        places[2 * dist - 1] = (a - dist, a >= dist)
        places[2 * dist] = (a + dist, a + dist < A)

    def near_copy(dy, slot, h):
        where = jnp.clip(places[slot][0], 0, A - 1)
        return forward((where, b), pl.ds(*cuts[h]), near_send.at[dy - 1, slot, h],
                       near_recv.at[dy - 1, slot, h], at(a, turn(y, dy, Y), c))

    def core_copy(dc, dy, slot, h):
        where = jnp.clip(places[slot][0], 0, A - 1)
        return forward((where, turn(y, -dy, Y) * C + c), pl.ds(*cuts[h]), core_send.at[dc - 1, dy, slot, h],
                       core_recv.at[dc - 1, dy, slot, h], at(a, y, turn(c, dc, C)))

    def to_near(slot, h):
        for dy in range(1, Y):
            near_copy(dy, slot, h).start()

    def to_core(dy, slot, h):
        for dc in range(1, C):
            core_copy(dc, dy, slot, h).start()

    def along(up, dist, h):
        there = jnp.minimum(a + dist, A - 1) if up else jnp.maximum(a - dist, 0)
        return forward((a, b), pl.ds(*cuts[h]), far_send.at[0 if up else 1, dist, h],
                       far_recv.at[0 if up else 1, dist, h], at(there, y, c))

    def spread(h, act="start"):
        for dist in range(A - 1, 0, -1):
            pl.when(a + dist < A)(lambda dist=dist: getattr(along(True, dist, h), act)())
            pl.when(a >= dist)(lambda dist=dist: getattr(along(False, dist, h), act)())

    first_fix = 1.0 / (1.0 - 0.9**STEP)
    second_fix = 1.0 / (1.0 - 0.95**STEP)
    for h, (at0, wide) in enumerate(cuts):
        cols = pl.ds(at0, wide)
        clipped = clip * part[A - 1, :, cols]
        m = 0.9 * first_v[:, cols] + 0.1 * clipped
        v = 0.95 * second_v[:, cols] + 0.05 * (clipped * clipped)
        d = (m * first_fix) / (jnp.sqrt(v * second_fix) + 1e-08)
        w = master_v[:, cols]
        w = w - 0.001 * (d + 0.1 * w)
        weights[a, b, :, cols] = w.astype(jnp.bfloat16)
        new_master[:, cols] = w
        new_first[:, cols] = m
        new_second[:, cols] = v
        direction[:, cols] = d
        spread(h)
        to_near(0, h)
        to_core(0, 0, h)

    def got_far(slot, h):
        dist = (slot + 1) // 2
        up = slot % 2 == 1
        block = weights.at[jnp.clip(places[slot][0], 0, A - 1), b, :, pl.ds(*cuts[h])]
        there = jnp.maximum(a - dist, 0) if up else jnp.minimum(a + dist, A - 1)
        pltpu.make_async_remote_copy(
            src_ref=block, dst_ref=block, send_sem=far_send.at[0 if up else 1, dist, h],
            recv_sem=far_recv.at[0 if up else 1, dist, h],
            device_id=at(there, y, c), device_id_type=MESH).wait_recv()
        to_near(slot, h)
        to_core(0, slot, h)

    def got_near(slot, h):
        for dy in range(1, Y):
            near_copy(dy, slot, h).wait_recv()
            to_core(dy, slot, h)

    def got_core(slot, h):
        for dc in range(1, C):
            for dy in range(Y):
                core_copy(dc, dy, slot, h).wait()
        for dy in range(1, Y):
            near_copy(dy, slot, h).wait_send()
        if slot == 0:
            spread(h, "wait_send")

    slots = sorted(places, key=lambda k: (k + 1) // 2)
    steps = [(slot, h) for h in range(len(cuts)) for slot in slots]
    lag = len(slots)

    def when(slot, work, h):
        if slot:
            pl.when(places[slot][1])(functools.partial(work, slot, h))
        else:
            work(slot, h)

    for i in range(len(steps) + lag):
        if i < len(steps) and steps[i][0]:
            when(steps[i][0], got_far, steps[i][1])
        if i >= lag:
            when(steps[i - lag][0], got_near, steps[i - lag][1])
    for slot, h in steps:
        when(slot, got_core, h)
    for copies in (raws, parts):
        for copy in copies.values():
            copy.wait_send()
    for copy in sent:
        copy.wait_send()


def write_out(*refs):
    count = len(refs) // 2
    copies = [pltpu.make_async_copy(refs[i], refs[count + i], refs[-1].at[i]) for i in range(count)]
    for copy in copies:
        copy.start()
    for copy in copies:
        copy.wait()


def solution(mesh):
    A, Y, C = factors(mesh)
    B = Y * C
    experts = mesh.shape["expert"]
    n = A * B

    def shards(grads, master, first_moment, second_moment):
        rows, width = master.shape[1:]
        H = len(pieces(width))
        dma = pltpu.SemaphoreType.DMA
        many = experts * n - 1
        vmem = pl.BlockSpec(memory_space=pltpu.VMEM)
        hbm = pl.BlockSpec(memory_space=pl.ANY)
        outs = pl.pallas_call(
            functools.partial(kernel, (A, Y, C), experts),
            out_shape=(pltpu.VMEM((rows, width), jnp.float32),) * 4 + (pltpu.VMEM((A, B, rows, width), jnp.bfloat16),),
            in_specs=[hbm] * 4,
            out_specs=(vmem,) * 5,
            scratch_shapes=[
                pltpu.VMEM((max(B - 1, 1), A, rows, width), jnp.bfloat16),
                pltpu.VMEM((A, rows, width), jnp.bfloat16),
                pltpu.VMEM((A, rows, width), jnp.float32),
                pltpu.VMEM((2, A, rows, width), jnp.float32),
                pltpu.VMEM((rows, width), jnp.float32),
                pltpu.VMEM((rows, width), jnp.float32),
                pltpu.VMEM((rows, width), jnp.float32),
                pltpu.VMEM((many + 1, 1, 128), jnp.float32),
                dma((4,)),
                dma((max(B - 1, 1), A, H)), dma((max(B - 1, 1), A, H)),
                dma((A, H)), dma((2, A, H)),
                dma((many,)), dma((many,)),
                dma((2, A, H)), dma((2, A, H)),
                dma((max(Y - 1, 1), 2 * A - 1, H)), dma((max(Y - 1, 1), 2 * A - 1, H)),
                dma((max(C - 1, 1), Y, 2 * A - 1, H)), dma((max(C - 1, 1), Y, 2 * A - 1, H)),
            ],
            compiler_params=pltpu.CompilerParams(collective_id=0, has_side_effects=True),
        )(grads.reshape(A, B, rows, width), master[0], first_moment[0], second_moment[0])
        outs = pl.pallas_call(
            write_out,
            out_shape=tuple(jax.ShapeDtypeStruct(x.shape, x.dtype) for x in outs),
            in_specs=[vmem] * 5,
            out_specs=(hbm,) * 5,
            scratch_shapes=[dma((5,))],
        )(*(pltpu.with_memory_space_constraint(x, pltpu.VMEM) for x in outs))
        return tuple(x[None] for x in outs[:4]) + (outs[4].reshape(1, n * rows, width),)

    split = P("expert", "dp", None)
    return jax.shard_map(shards, mesh=mesh, in_specs=(P("expert", "dp", None, None), split, split, split),
                         out_specs=(split, split, split, split, P("expert", None, None)), check_vma=False)
```

```python
import functools

import jax
import jax.numpy as jnp
from jax import lax
from jax.experimental import pallas as pl
from jax.experimental.pallas import tpu as pltpu
from jax.sharding import PartitionSpec as P

STEP = 10
CUTS = 2
GATHER_CUTS = 2
MESH = pl.DeviceIdType.MESH


def factors(mesh):
    size = mesh.shape["dp"]
    row = mesh.devices.reshape(-1, size)[0]
    try:
        places = [tuple(d.coords) for d in row]
        cores = size // len(set(places))
        far = len({p[2] for p in places})
    except AttributeError:
        cores, far = 1, size
    return far, size // far // cores, cores


def pieces(width, count):
    tiles = width // 128
    edges = [tiles * i // count * 128 for i in range(count)] + [width]
    return [(p, q - p) for p, q in zip(edges, edges[1:]) if q > p]


def kernel(sizes, experts, grads, master, first, second, new_master, new_first, new_second, direction, weights,
           raw, own, part, arrived, master_v, first_v, second_v, norms,
           load_sem, raw_send, raw_recv, part_send, part_recv, norm_send, norm_recv,
           far_send, far_recv, near_send, near_recv, core_send, core_recv):
    A, Y, C = sizes
    B = Y * C
    n = A * B
    width = grads.shape[-1]
    cuts, gcuts = pieces(width, CUTS), pieces(width, GATHER_CUTS)
    e, me = lax.axis_index("expert"), lax.axis_index("dp")
    a, b = me // B, me % B
    y, c = b // C, b % C

    def turn(value, by, count):
        return (value + by) % count

    def at(za, yb, cc):
        return (e, za * B + yb * C + cc)

    inner = [(dy, dc) for dy in range(Y) for dc in range(C) if dy or dc]
    inner.sort(key=lambda t: -t[0])
    table = [sorted(range(A), key=lambda t: (-abs(t - z), t)) for z in range(A)]

    def chosen(row):
        pick = row[0]
        for z in range(1, A):
            pick = jnp.where(a == z, row[z], pick)
        return pick

    targets = [chosen([table[z][s] for z in range(A)]) for s in range(A - 1)] + [a]
    everyone = [(de, dd) for de in range(experts) for dd in range(n) if de or dd]

    barrier = pltpu.get_barrier_semaphore()

    def greet(device):
        pl.semaphore_signal(barrier, inc=1, device_id=device, device_id_type=MESH)

    for dy, dc in inner:
        greet(at(a, turn(y, dy, Y), turn(c, dc, C)))
    for de in range(1, experts):
        greet((turn(e, de, experts), me))
    pl.when(a > 0)(lambda: greet(at(a - 1, y, c)))
    pl.when(a < A - 1)(lambda: greet(at(a + 1, y, c)))
    greeted = len(inner) + experts - 1 + jnp.where(a > 0, 1, 0) + jnp.where(a < A - 1, 1, 0)

    loads = [pltpu.make_async_copy(grads.at[:, b], own, load_sem.at[0])]
    for i, (src, dst) in enumerate(((master, master_v), (first, first_v), (second, second_v))):
        loads.append(pltpu.make_async_copy(src, dst, load_sem.at[i + 1]))
    for copy in loads:
        copy.start()
    pl.semaphore_wait(barrier, greeted)

    raws = {}
    for s, t in enumerate(targets):
        for h, (at0, wide) in enumerate(cuts):
            for i, (dy, dc) in enumerate(inner):
                y2, c2 = turn(y, dy, Y), turn(c, dc, C)
                copy = pltpu.make_async_remote_copy(
                    src_ref=grads.at[t, y2 * C + c2, :, pl.ds(at0, wide)],
                    dst_ref=raw.at[i, s, :, pl.ds(at0, wide)],
                    send_sem=raw_send.at[i, s, h], recv_sem=raw_recv.at[i, s, h],
                    device_id=at(a, y2, c2), device_id_type=MESH)
                copy.start()
                raws[i, s, h] = copy
    loads[0].wait()

    def step_on(d, s, t, h):
        cols = pl.ds(*cuts[h])
        ahead = jnp.where(d == 0, jnp.minimum(a + 1, A - 1), jnp.maximum(a - 1, 0))
        return pltpu.make_async_remote_copy(
            src_ref=part.at[s, :, cols], dst_ref=arrived.at[d, t, :, cols],
            send_sem=part_send.at[s, h], recv_sem=part_recv.at[d, t, h],
            device_id=at(ahead, y, c), device_id_type=MESH)

    def add_arrived(d, s, t, h):
        cols = pl.ds(*cuts[h])
        step_on(d, s, t, h).wait_recv()
        part[s, :, cols] = part[s, :, cols] + arrived[d, t, :, cols]

    parts = {}
    square = jnp.zeros((1, 128), jnp.float32)
    for s, t in enumerate(targets):
        for h, (at0, wide) in enumerate(cuts):
            cols = pl.ds(at0, wide)
            total = own[t, :, cols].astype(jnp.float32)
            for i in range(len(inner)):
                raws[i, s, h].wait_recv()
                total = total + raw[i, s, :, cols].astype(jnp.float32)
            part[s, :, cols] = total
            if s < A - 1:
                d = jnp.where(t > a, 0, 1)
                behind = jnp.where(t > a, a, A - 1 - a)
                pl.when(behind > 0)(functools.partial(add_arrived, d, s, t, h))
                parts[s, h] = step_on(d, s, t, h)
                parts[s, h].start()
            else:
                pl.when(a > 0)(functools.partial(add_arrived, 0, s, t, h))
                pl.when(a < A - 1)(functools.partial(add_arrived, 1, s, t, h))
                total = part[s, :, cols]
                squares = jnp.sum(total * total, axis=0, keepdims=True)
                for j in range(wide // 128):
                    square = square + squares[:, j * 128:(j + 1) * 128]
    norms[0] = square
    sent = []
    for i, (de, dd) in enumerate(everyone):
        copy = pltpu.make_async_remote_copy(
            src_ref=norms.at[0], dst_ref=norms.at[i + 1],
            send_sem=norm_send.at[i], recv_sem=norm_recv.at[i],
            device_id=(turn(e, de, experts), turn(me, dd, n)), device_id_type=MESH)
        copy.start()
        sent.append(copy)
    for copy in loads[1:]:
        copy.wait()
    for copy in sent:
        copy.wait_recv()
    whole = jnp.sum(jnp.sum(norms[...], axis=0), axis=1, keepdims=True)
    clip = 1.0 / jnp.maximum(jnp.sqrt(whole), 1.0)

    def forward(where, cols, send, recv, target):
        copy = pltpu.make_async_remote_copy(
            src_ref=weights.at[where[0], where[1], :, cols], dst_ref=weights.at[where[0], where[1], :, cols],
            send_sem=send, recv_sem=recv, device_id=target, device_id_type=MESH)
        return copy

    places = {0: (a, True)}
    for dist in range(1, A):
        places[2 * dist - 1] = (a - dist, a >= dist)
        places[2 * dist] = (a + dist, a + dist < A)

    def near_copy(dy, slot, h):
        where = jnp.clip(places[slot][0], 0, A - 1)
        return forward((where, b), pl.ds(*gcuts[h]), near_send.at[dy - 1, slot, h],
                       near_recv.at[dy - 1, slot, h], at(a, turn(y, dy, Y), c))

    def core_copy(dc, dy, slot, h):
        where = jnp.clip(places[slot][0], 0, A - 1)
        return forward((where, turn(y, -dy, Y) * C + c), pl.ds(*gcuts[h]), core_send.at[dc - 1, dy, slot, h],
                       core_recv.at[dc - 1, dy, slot, h], at(a, y, turn(c, dc, C)))

    def to_near(slot, h):
        for dy in range(1, Y):
            near_copy(dy, slot, h).start()

    def to_core(dy, slot, h):
        for dc in range(1, C):
            core_copy(dc, dy, slot, h).start()

    def along(slot, up, hop, h):
        dist = (slot + 1) // 2 + hop
        where = jnp.clip(places[slot][0], 0, A - 1)
        there = jnp.minimum(a + hop, A - 1) if up else jnp.maximum(a - hop, 0)
        return pltpu.make_async_remote_copy(
            src_ref=weights.at[where, b, :, pl.ds(*gcuts[h])], dst_ref=weights.at[where, b, :, pl.ds(*gcuts[h])],
            send_sem=far_send.at[0 if up else 1, dist, h], recv_sem=far_recv.at[0 if up else 1, dist, h],
            device_id=at(there, y, c), device_id_type=MESH)

    def relay(slot, up, h, act="start", hops=(2, 1)):
        dist = (slot + 1) // 2
        if dist % 2:
            return
        for hop in hops:
            if dist + hop < A:
                here = (a + hop < A) if up else (a - hop >= 0)
                pl.when(here)(lambda hop=hop: getattr(along(slot, up, hop, h), act)())

    first_fix = 1.0 / (1.0 - 0.9**STEP)
    second_fix = 1.0 / (1.0 - 0.95**STEP)
    for h, (at0, wide) in enumerate(cuts):
        cols = pl.ds(at0, wide)
        clipped = clip * part[A - 1, :, cols]
        m = 0.9 * first_v[:, cols] + 0.1 * clipped
        v = 0.95 * second_v[:, cols] + 0.05 * (clipped * clipped)
        d = (m * first_fix) / (jnp.sqrt(v * second_fix) + 1e-08)
        w = master_v[:, cols]
        w = w - 0.001 * (d + 0.1 * w)
        weights[a, b, :, cols] = w.astype(jnp.bfloat16)
        new_master[:, cols] = w
        new_first[:, cols] = m
        new_second[:, cols] = v
        direction[:, cols] = d
    for h in range(len(gcuts)):
        relay(0, True, h)
        relay(0, False, h)
        to_near(0, h)
    for h in range(len(gcuts)):
        to_core(0, 0, h)

    def got_far(slot, h):
        dist = (slot + 1) // 2
        up = slot % 2 == 1
        hop = 1 if dist % 2 else 2
        block = weights.at[jnp.clip(places[slot][0], 0, A - 1), b, :, pl.ds(*gcuts[h])]
        there = jnp.maximum(a - hop, 0) if up else jnp.minimum(a + hop, A - 1)
        pltpu.make_async_remote_copy(
            src_ref=block, dst_ref=block, send_sem=far_send.at[0 if up else 1, dist, h],
            recv_sem=far_recv.at[0 if up else 1, dist, h],
            device_id=at(there, y, c), device_id_type=MESH).wait_recv()
        relay(slot, up, h)
        to_near(slot, h)
        to_core(0, slot, h)

    def got_near(slot, h):
        for dy in range(1, Y):
            near_copy(dy, slot, h).wait_recv()
            to_core(dy, slot, h)

    def got_core(slot, h):
        for dc in range(1, C):
            for dy in range(Y):
                core_copy(dc, dy, slot, h).wait()
        for dy in range(1, Y):
            near_copy(dy, slot, h).wait_send()
        if slot == 0 or slot % 2:
            relay(slot, True, h, "wait_send")
        if slot % 2 == 0:
            relay(slot, False, h, "wait_send")

    slots = sorted(places, key=lambda k: (k + 1) // 2)
    ranks = [(slot, h) for h in range(len(gcuts)) for slot in slots]
    steps = sorted(ranks, key=lambda r: ((r[0] + 1) // 2 > 2, r[1], -((r[0] + 1) // 2) % 3))
    lag = len(slots)

    def when(slot, work, h):
        if slot:
            pl.when(places[slot][1])(functools.partial(work, slot, h))
        else:
            work(slot, h)

    for i in range(len(steps) + lag):
        if i < len(steps) and steps[i][0]:
            when(steps[i][0], got_far, steps[i][1])
        if i >= lag:
            when(steps[i - lag][0], got_near, steps[i - lag][1])
    for slot, h in steps:
        when(slot, got_core, h)
    for copies in (raws, parts):
        for copy in copies.values():
            copy.wait_send()
    for copy in sent:
        copy.wait_send()


def write_out(*refs):
    count = len(refs) // 2
    copies = [pltpu.make_async_copy(refs[i], refs[count + i], refs[-1].at[i]) for i in range(count)]
    for copy in copies:
        copy.start()
    for copy in copies:
        copy.wait()


def solution(mesh):
    A, Y, C = factors(mesh)
    B = Y * C
    experts = mesh.shape["expert"]
    n = A * B

    def shards(grads, master, first_moment, second_moment):
        rows, width = master.shape[1:]
        H, G = len(pieces(width, CUTS)), len(pieces(width, GATHER_CUTS))
        dma = pltpu.SemaphoreType.DMA
        many = experts * n - 1
        vmem = pl.BlockSpec(memory_space=pltpu.VMEM)
        hbm = pl.BlockSpec(memory_space=pl.ANY)
        outs = pl.pallas_call(
            functools.partial(kernel, (A, Y, C), experts),
            out_shape=(pltpu.VMEM((rows, width), jnp.float32),) * 4 + (pltpu.VMEM((A, B, rows, width), jnp.bfloat16),),
            in_specs=[hbm] * 4,
            out_specs=(vmem,) * 5,
            scratch_shapes=[
                pltpu.VMEM((max(B - 1, 1), A, rows, width), jnp.bfloat16),
                pltpu.VMEM((A, rows, width), jnp.bfloat16),
                pltpu.VMEM((A, rows, width), jnp.float32),
                pltpu.VMEM((2, A, rows, width), jnp.float32),
                pltpu.VMEM((rows, width), jnp.float32),
                pltpu.VMEM((rows, width), jnp.float32),
                pltpu.VMEM((rows, width), jnp.float32),
                pltpu.VMEM((many + 1, 1, 128), jnp.float32),
                dma((4,)),
                dma((max(B - 1, 1), A, H)), dma((max(B - 1, 1), A, H)),
                dma((A, H)), dma((2, A, H)),
                dma((many,)), dma((many,)),
                dma((2, A, G)), dma((2, A, G)),
                dma((max(Y - 1, 1), 2 * A - 1, G)), dma((max(Y - 1, 1), 2 * A - 1, G)),
                dma((max(C - 1, 1), Y, 2 * A - 1, G)), dma((max(C - 1, 1), Y, 2 * A - 1, G)),
            ],
            compiler_params=pltpu.CompilerParams(collective_id=0, has_side_effects=True),
        )(grads.reshape(A, B, rows, width), master[0], first_moment[0], second_moment[0])
        outs = pl.pallas_call(
            write_out,
            out_shape=tuple(jax.ShapeDtypeStruct(x.shape, x.dtype) for x in outs),
            in_specs=[vmem] * 5,
            out_specs=(hbm,) * 5,
            scratch_shapes=[dma((5,))],
        )(*(pltpu.with_memory_space_constraint(x, pltpu.VMEM) for x in outs))
        return tuple(x[None] for x in outs[:4]) + (outs[4].reshape(1, n * rows, width),)

    split = P("expert", "dp", None)
    return jax.shard_map(shards, mesh=mesh, in_specs=(P("expert", "dp", None, None), split, split, split),
                         out_specs=(split, split, split, split, P("expert", None, None)), check_vma=False)
```

```python
import functools

import jax
import jax.numpy as jnp
from jax import lax
from jax.experimental import pallas as pl
from jax.experimental.pallas import tpu as pltpu
from jax.sharding import PartitionSpec as P

STEP = 10
CUTS = 2
GATHER_CUTS = 2
MESH = pl.DeviceIdType.MESH


def factors(mesh):
    size = mesh.shape["dp"]
    row = mesh.devices.reshape(-1, size)[0]
    try:
        places = [tuple(d.coords) for d in row]
        cores = size // len(set(places))
        far = len({p[2] for p in places})
    except AttributeError:
        cores, far = 1, size
    return far, size // far // cores, cores


def pieces(width, count):
    tiles = width // 128
    edges = [tiles * i // count * 128 for i in range(count)] + [width]
    return [(p, q - p) for p, q in zip(edges, edges[1:]) if q > p]


def kernel(sizes, experts, grads, master, first, second, new_master, new_first, new_second, direction, weights,
           raw, own, part, arrived, master_v, first_v, second_v, norms,
           load_sem, raw_send, raw_recv, part_send, part_recv, norm_send, norm_recv,
           far_send, far_recv, near_send, near_recv, core_send, core_recv):
    A, Y, C = sizes
    B = Y * C
    n = A * B
    width = grads.shape[-1]
    cuts, gcuts = pieces(width, CUTS), pieces(width, GATHER_CUTS)
    e, me = lax.axis_index("expert"), lax.axis_index("dp")
    a, b = me // B, me % B
    y, c = b // C, b % C

    def turn(value, by, count):
        later = value + by % count
        return later if by % count == 0 else jnp.where(later >= count, later - count, later)

    ys, cs = [turn(y, dy, Y) for dy in range(Y)], [turn(c, dc, C) for dc in range(C)]

    def at(za, yb, cc):
        return (e, za * B + yb * C + cc)

    inner = [(dy, dc) for dy in range(Y) for dc in range(C) if dy or dc]
    inner.sort(key=lambda t: -t[0])
    table = [sorted(range(A), key=lambda t: (-abs(t - z), t)) for z in range(A)]

    def chosen(row):
        pick = row[0]
        for z in range(1, A):
            pick = jnp.where(a == z, row[z], pick)
        return pick

    targets = [chosen([table[z][s] for z in range(A)]) for s in range(A - 1)] + [a]
    everyone = [(de, dd) for de in range(experts) for dd in range(n) if de or dd]

    barrier = pltpu.get_barrier_semaphore()

    def greet(device):
        pl.semaphore_signal(barrier, inc=1, device_id=device, device_id_type=MESH)

    for dy, dc in inner:
        greet(at(a, ys[dy], cs[dc]))
    for de in range(1, experts):
        greet((turn(e, de, experts), me))
    pl.when(a > 0)(lambda: greet(at(a - 1, y, c)))
    pl.when(a < A - 1)(lambda: greet(at(a + 1, y, c)))
    greeted = len(inner) + experts - 1 + jnp.where(a > 0, 1, 0) + jnp.where(a < A - 1, 1, 0)

    loads = [pltpu.make_async_copy(grads.at[:, b], own, load_sem.at[0])]
    for i, (src, dst) in enumerate(((master, master_v), (first, first_v), (second, second_v))):
        loads.append(pltpu.make_async_copy(src, dst, load_sem.at[i + 1]))
    for copy in loads:
        copy.start()
    pl.semaphore_wait(barrier, greeted)

    raws = {}
    for s, t in enumerate(targets):
        for h, (at0, wide) in enumerate(cuts):
            for i, (dy, dc) in enumerate(inner):
                y2, c2 = ys[dy], cs[dc]
                copy = pltpu.make_async_remote_copy(
                    src_ref=grads.at[t, y2 * C + c2, :, pl.ds(at0, wide)],
                    dst_ref=raw.at[i, s, :, pl.ds(at0, wide)],
                    send_sem=raw_send.at[i, s, h], recv_sem=raw_recv.at[i, s, h],
                    device_id=at(a, y2, c2), device_id_type=MESH)
                copy.start()
                raws[i, s, h] = copy
    loads[0].wait()

    def step_on(d, s, t, h):
        cols = pl.ds(*cuts[h])
        ahead = jnp.where(d == 0, jnp.minimum(a + 1, A - 1), jnp.maximum(a - 1, 0))
        return pltpu.make_async_remote_copy(
            src_ref=part.at[s, :, cols], dst_ref=arrived.at[d, t, :, cols],
            send_sem=part_send.at[s, h], recv_sem=part_recv.at[d, t, h],
            device_id=at(ahead, y, c), device_id_type=MESH)

    def add_arrived(d, s, t, h):
        cols = pl.ds(*cuts[h])
        step_on(d, s, t, h).wait_recv()
        part[s, :, cols] = part[s, :, cols] + arrived[d, t, :, cols]

    parts = {}
    square = jnp.zeros((1, 128), jnp.float32)
    for s, t in enumerate(targets):
        for h, (at0, wide) in enumerate(cuts):
            cols = pl.ds(at0, wide)
            total = own[t, :, cols].astype(jnp.float32)
            for i in range(len(inner)):
                raws[i, s, h].wait_recv()
                total = total + raw[i, s, :, cols].astype(jnp.float32)
            part[s, :, cols] = total
            if s < A - 1:
                d = jnp.where(t > a, 0, 1)
                behind = jnp.where(t > a, a, A - 1 - a)
                pl.when(behind > 0)(functools.partial(add_arrived, d, s, t, h))
                parts[s, h] = step_on(d, s, t, h)
                parts[s, h].start()
            else:
                pl.when(a > 0)(functools.partial(add_arrived, 0, s, t, h))
                pl.when(a < A - 1)(functools.partial(add_arrived, 1, s, t, h))
                total = part[s, :, cols]
                squares = jnp.sum(total * total, axis=0, keepdims=True)
                for j in range(wide // 128):
                    square = square + squares[:, j * 128:(j + 1) * 128]
    norms[0] = square
    sent = []
    for i, (de, dd) in enumerate(everyone):
        copy = pltpu.make_async_remote_copy(
            src_ref=norms.at[0], dst_ref=norms.at[i + 1],
            send_sem=norm_send.at[i], recv_sem=norm_recv.at[i],
            device_id=(turn(e, de, experts), turn(me, dd, n)), device_id_type=MESH)
        copy.start()
        sent.append(copy)
    for copy in loads[1:]:
        copy.wait()
    for copy in sent:
        copy.wait_recv()
    whole = jnp.sum(jnp.sum(norms[...], axis=0), axis=1, keepdims=True)
    clip = 1.0 / jnp.maximum(jnp.sqrt(whole), 1.0)

    def forward(where, cols, send, recv, target):
        copy = pltpu.make_async_remote_copy(
            src_ref=weights.at[where[0], where[1], :, cols], dst_ref=weights.at[where[0], where[1], :, cols],
            send_sem=send, recv_sem=recv, device_id=target, device_id_type=MESH)
        return copy

    places = {0: (a, True)}
    for dist in range(1, A):
        places[2 * dist - 1] = (jnp.maximum(a - dist, 0), a >= dist)
        places[2 * dist] = (jnp.minimum(a + dist, A - 1), a + dist < A)

    def near_copy(dy, slot, h):
        where = places[slot][0]
        return forward((where, b), pl.ds(*gcuts[h]), near_send.at[dy - 1, slot, h],
                       near_recv.at[dy - 1, slot, h], at(a, ys[dy], c))

    def core_copy(dc, dy, slot, h):
        where = places[slot][0]
        return forward((where, ys[-dy % Y] * C + c), pl.ds(*gcuts[h]), core_send.at[dc - 1, dy, slot, h],
                       core_recv.at[dc - 1, dy, slot, h], at(a, y, cs[dc]))

    def to_near(slot, h):
        for dy in range(1, Y):
            near_copy(dy, slot, h).start()

    def to_core(dy, slot, h):
        for dc in range(1, C):
            core_copy(dc, dy, slot, h).start()

    def along(slot, up, hop, h):
        dist = (slot + 1) // 2 + hop
        where = places[slot][0]
        there = jnp.minimum(a + hop, A - 1) if up else jnp.maximum(a - hop, 0)
        return pltpu.make_async_remote_copy(
            src_ref=weights.at[where, b, :, pl.ds(*gcuts[h])], dst_ref=weights.at[where, b, :, pl.ds(*gcuts[h])],
            send_sem=far_send.at[0 if up else 1, dist, h], recv_sem=far_recv.at[0 if up else 1, dist, h],
            device_id=at(there, y, c), device_id_type=MESH)

    def relay(slot, up, h, act="start", hops=(2, 1)):
        dist = (slot + 1) // 2
        if dist % 2:
            return
        for hop in hops:
            if dist + hop < A:
                here = (a + hop < A) if up else (a - hop >= 0)
                pl.when(here)(lambda hop=hop: getattr(along(slot, up, hop, h), act)())

    first_fix = 1.0 / (1.0 - 0.9**STEP)
    second_fix = 1.0 / (1.0 - 0.95**STEP)
    for h, (at0, wide) in enumerate(gcuts):
        cols = pl.ds(at0, wide)
        clipped = clip * part[A - 1, :, cols]
        m = 0.9 * first_v[:, cols] + 0.1 * clipped
        v = 0.95 * second_v[:, cols] + 0.05 * (clipped * clipped)
        d = (m * first_fix) / (jnp.sqrt(v * second_fix) + 1e-08)
        w = master_v[:, cols]
        w = w - 0.001 * (d + 0.1 * w)
        weights[a, b, :, cols] = w.astype(jnp.bfloat16)
        new_master[:, cols] = w
        new_first[:, cols] = m
        new_second[:, cols] = v
        direction[:, cols] = d
        relay(0, True, h)
        relay(0, False, h)
        to_near(0, h)
    for h in range(len(gcuts)):
        to_core(0, 0, h)

    def got_far(slot, h):
        dist = (slot + 1) // 2
        up = slot % 2 == 1
        hop = 1 if dist % 2 else 2
        block = weights.at[places[slot][0], b, :, pl.ds(*gcuts[h])]
        there = jnp.maximum(a - hop, 0) if up else jnp.minimum(a + hop, A - 1)
        pltpu.make_async_remote_copy(
            src_ref=block, dst_ref=block, send_sem=far_send.at[0 if up else 1, dist, h],
            recv_sem=far_recv.at[0 if up else 1, dist, h],
            device_id=at(there, y, c), device_id_type=MESH).wait_recv()
        relay(slot, up, h)
        to_near(slot, h)
        to_core(0, slot, h)

    def got_near(slot, h):
        for dy in range(1, Y):
            near_copy(dy, slot, h).wait_recv()
            to_core(dy, slot, h)

    def got_core(slot, h):
        for dc in range(1, C):
            for dy in range(Y):
                core_copy(dc, dy, slot, h).wait()
        for dy in range(1, Y):
            near_copy(dy, slot, h).wait_send()
        if slot == 0 or slot % 2:
            relay(slot, True, h, "wait_send")
        if slot % 2 == 0:
            relay(slot, False, h, "wait_send")

    slots = sorted(places, key=lambda k: (k + 1) // 2)
    ranks = [(slot, h) for h in range(len(gcuts)) for slot in slots]
    steps = sorted(ranks, key=lambda r: ((r[0] + 1) // 2 > 2, r[1], -((r[0] + 1) // 2) % 3))
    lag = len(steps)

    def when(slot, work, h):
        if slot:
            pl.when(places[slot][1])(functools.partial(work, slot, h))
        else:
            work(slot, h)

    for i in range(len(steps) + lag):
        if i < len(steps) and steps[i][0]:
            when(steps[i][0], got_far, steps[i][1])
        if i >= lag:
            when(steps[i - lag][0], got_near, steps[i - lag][1])
    for slot, h in steps:
        when(slot, got_core, h)
    for copies in (raws, parts):
        for copy in copies.values():
            copy.wait_send()
    for copy in sent:
        copy.wait_send()


def write_out(*refs):
    count = len(refs) // 2
    copies = [pltpu.make_async_copy(refs[i], refs[count + i], refs[-1].at[i]) for i in range(count)]
    for copy in copies:
        copy.start()
    for copy in copies:
        copy.wait()


def solution(mesh):
    A, Y, C = factors(mesh)
    B = Y * C
    experts = mesh.shape["expert"]
    n = A * B

    def shards(grads, master, first_moment, second_moment):
        rows, width = master.shape[1:]
        H, G = len(pieces(width, CUTS)), len(pieces(width, GATHER_CUTS))
        dma = pltpu.SemaphoreType.DMA
        many = experts * n - 1
        vmem = pl.BlockSpec(memory_space=pltpu.VMEM)
        hbm = pl.BlockSpec(memory_space=pl.ANY)
        outs = pl.pallas_call(
            functools.partial(kernel, (A, Y, C), experts),
            out_shape=(pltpu.VMEM((rows, width), jnp.float32),) * 4 + (pltpu.VMEM((A, B, rows, width), jnp.bfloat16),),
            in_specs=[hbm] * 4,
            out_specs=(vmem,) * 5,
            scratch_shapes=[
                pltpu.VMEM((max(B - 1, 1), A, rows, width), jnp.bfloat16),
                pltpu.VMEM((A, rows, width), jnp.bfloat16),
                pltpu.VMEM((A, rows, width), jnp.float32),
                pltpu.VMEM((2, A, rows, width), jnp.float32),
                pltpu.VMEM((rows, width), jnp.float32),
                pltpu.VMEM((rows, width), jnp.float32),
                pltpu.VMEM((rows, width), jnp.float32),
                pltpu.VMEM((many + 1, 1, 128), jnp.float32),
                dma((4,)),
                dma((max(B - 1, 1), A, H)), dma((max(B - 1, 1), A, H)),
                dma((A, H)), dma((2, A, H)),
                dma((many,)), dma((many,)),
                dma((2, A, G)), dma((2, A, G)),
                dma((max(Y - 1, 1), 2 * A - 1, G)), dma((max(Y - 1, 1), 2 * A - 1, G)),
                dma((max(C - 1, 1), Y, 2 * A - 1, G)), dma((max(C - 1, 1), Y, 2 * A - 1, G)),
            ],
            compiler_params=pltpu.CompilerParams(collective_id=0, has_side_effects=True),
        )(grads.reshape(A, B, rows, width), master[0], first_moment[0], second_moment[0])
        outs = pl.pallas_call(
            write_out,
            out_shape=tuple(jax.ShapeDtypeStruct(x.shape, x.dtype) for x in outs),
            in_specs=[vmem] * 5,
            out_specs=(hbm,) * 5,
            scratch_shapes=[dma((5,))],
        )(*(pltpu.with_memory_space_constraint(x, pltpu.VMEM) for x in outs))
        return tuple(x[None] for x in outs[:4]) + (outs[4].reshape(1, n * rows, width),)

    split = P("expert", "dp", None)
    return jax.shard_map(shards, mesh=mesh, in_specs=(P("expert", "dp", None, None), split, split, split),
                         out_specs=(split, split, split, split, P("expert", None, None)), check_vma=False)
```
